128 devices in a mesh: grp: 4 (over y_lo, core), dev: 32 (over z, x, y_hi).
Axes of the slice: x: 4, y: 4 (y_hi: 2, y_lo: 2; y = y_hi * 2 + y_lo), z: 4, core: 2. Of those that a mesh axis runs over, the one named last changes fastest.
Arguments:
- targets: float32 [64, 65536], P(None, ('grp', 'dev')), may hold values from -1.7 to 1.7
- source_grid: int32 [64, 16384], P(None, ('grp', 'dev')), may hold values from -1331000 to 1331000
- source_weight: int32 [1, 16384], P(None, ('grp', 'dev')), may hold values from 1 to 1024
Outputs:
- kernel_sum: float32 [65536], P(('grp', 'dev'))
The draws below stay inside these ranges and needn't reach their ends.
All inputs are finite; a program needn't handle non-finite values.
Results may differ from the reference program's by a relative error of at most 0.00017.
Values sent between devices are 32-bit elements; how exact they have to be, the bound alone decides.
A program may use at most 64 MiB of HBM per device.

```python
import jax
import jax.numpy as jnp
from jax import lax

D = 64
TGT_DEV = 512
SRC_DEV = 128
TARGETS = 65536
SOURCES = 16384
N_DEV = 32


def centre_table(key):
    centre_count = max(SOURCES // SRC_DEV, 1)
    return jax.random.randint(jax.random.fold_in(key, 11), (D, centre_count), -495000, 495001)


def draw_source_grid(key, part):
    centre_count = max(SOURCES // SRC_DEV, 1)
    centres = centre_table(key)
    owner = jax.random.permutation(jax.random.fold_in(key, 12), SOURCES) % centre_count
    first_noise = jax.random.randint(jax.random.fold_in(key, 13), (D, SOURCES), -418000, 418001)
    second_noise = jax.random.randint(jax.random.fold_in(key, 14), (D, SOURCES), -418000, 418001)
    return (centres[:, owner] + first_noise + second_noise).astype(jnp.int32)


def draw_targets(key, part):
    centre_count = max(SOURCES // SRC_DEV, 1)
    centres = centre_table(key).astype(jnp.float32) / 1048576.0
    owner = jax.random.randint(jax.random.fold_in(key, 15), (TARGETS,), 0, centre_count)
    base = centres[:, owner]
    noise = jnp.clip(0.326 * jax.random.normal(jax.random.fold_in(key, 17), (D, TARGETS), jnp.float32), -1.2, 1.2)
    return (base + noise).astype(jnp.float32)


def place_ends(values, key, smallest, top_value):
    index_at = [jax.random.randint(jax.random.fold_in(key, axis), (), 0, length) for axis, length in enumerate(values.shape)]
    widest = values.shape.index(max(values.shape))
    neighbour = index_at[:widest] + [(index_at[widest] + 1) % values.shape[widest]] + index_at[widest + 1:]
    return values.at[tuple(index_at)].set(smallest).at[tuple(neighbour)].set(top_value)


def setup_inputs(seed: int = 0) -> dict:
    arg_keys = jax.random.split(jax.random.key(seed), 4)
    return {
        "targets": draw_targets(jax.random.fold_in(arg_keys[3], 71), 0),
        "source_grid": draw_source_grid(jax.random.fold_in(arg_keys[3], 71), 0),
        "source_weight": place_ends(jax.random.randint(arg_keys[2], (1, SOURCES), 1, 1025), jax.random.fold_in(arg_keys[2], 1), 1, 1024).astype(jnp.int32),
    }


KERNEL_RATE = 0.7


def block_sum(tgt_rows, src_points, src_mass):
    tgt_norm = jnp.sum(tgt_rows * tgt_rows, axis=0)
    src_norm = jnp.sum(src_points * src_points, axis=0)
    inner_prod = lax.dot_general(tgt_rows, src_points, (((0,), (0,)), ((), ())), precision=lax.Precision.HIGHEST, preferred_element_type=jnp.float32)
    distance = tgt_norm[:, None] + src_norm[None, :] - 2.0 * inner_prod
    kernel = jnp.exp(-KERNEL_RATE * distance)
    return jnp.dot(kernel, src_mass[0], precision=lax.Precision.HIGHEST, preferred_element_type=jnp.float32)


def reference(targets, source_grid, source_weight):
    points = source_grid.astype(jnp.float32) / 1048576.0
    masses = source_weight.astype(jnp.float32) / 16.0
    rows_block = TGT_DEV * min(8, N_DEV)
    cols_block = SRC_DEV * 4
    count_cols = SOURCES // cols_block
    point_blocks = jnp.transpose(points.reshape(D, count_cols, cols_block), (1, 0, 2))
    mass_blocks = jnp.transpose(masses.reshape(1, count_cols, cols_block), (1, 0, 2))
    target_blocks = jnp.transpose(targets.reshape(D, TARGETS // rows_block, rows_block), (1, 0, 2))

    def one_target_block(tgt_rows):
        def advance(running, source_pair):
            return running + block_sum(tgt_rows, source_pair[0], source_pair[1]), None
        result, unused = lax.scan(advance, jnp.zeros((rows_block,), jnp.float32), (point_blocks, mass_blocks))
        return result

    sums = lax.map(one_target_block, target_blocks)
    return sums.reshape(TARGETS)
```

```python
import functools
import math

import jax
import jax.numpy as jnp
from jax import lax
from jax.experimental import pallas as pl
from jax.experimental.pallas import tpu as pltpu
from jax.sharding import PartitionSpec as P

KERNEL_RATE = 0.7
RATE2 = KERNEL_RATE * math.log2(math.e)
MESH = pl.DeviceIdType.MESH
DMA = pltpu.SemaphoreType.DMA
f32, bf16, i32 = jnp.float32, jnp.bfloat16, jnp.int32

D, TGT, SRC = 64, 512, 128
PLANE = [(dx, dy) for dx in range(4) for dy in range(4) if dx or dy]
ORDER = [(0, 0), (1, 0), (3, 0), (0, 1), (0, 3), (1, 1), (3, 1), (1, 3), (3, 3), (2, 0), (0, 2), (2, 1), (2, 3), (1, 2), (3, 2), (2, 2)]
ZS = (2, 1, 3)
GROUPS, PER = 4, 4


def coords():
    g, d = lax.axis_index("grp"), lax.axis_index("dev")
    return lax.div(d, 8), lax.rem(lax.div(d, 2), 4), 2 * lax.rem(d, 2) + lax.div(g, 2), lax.rem(g, 2)


def peer(me, dz=0, dx=0, dy=0, dc=0):
    z, x, y, c = (lax.rem(a + b, n) for a, b, n in zip(me, (dz, dx, dy, dc), (4, 4, 4, 2)))
    return (lax.rem(y, 2) * 2 + c, z * 8 + x * 2 + lax.div(y, 2))


def ext_rows(v, first):
    a = v.astype(bf16).astype(f32)
    b = (v - a).astype(bf16).astype(f32)
    c = v - a - b
    row = lax.broadcasted_iota(i32, (8, v.shape[1]), 0)
    k, o = (0, 3) if first else (3, 0)
    ones = jnp.where((row >= o) & (row < o + 3), 1.0, 0.0)
    rows = jnp.where(row == k, a, jnp.where(row == k + 1, b, jnp.where(row == k + 2, c, ones)))
    return jnp.concatenate([rows, jnp.zeros((D - 8, v.shape[1]), f32)], 0).astype(bf16)


def split(v):
    hi = v.astype(bf16)
    return hi, (v - hi.astype(f32)).astype(bf16)


def prep_targets(t):
    norm = -RATE2 * jnp.sum(t * t, axis=0, keepdims=True)
    hi, lo = split(t * (2.0 * RATE2))
    return jnp.concatenate([hi, hi, lo, ext_rows(norm, False)], 0)


def prep_sources(grid, weight):
    p = grid.astype(f32) * (1.0 / 1048576.0)
    bias = jnp.log2(weight.astype(f32) * (1.0 / 16.0)) - RATE2 * jnp.sum(p * p, axis=0, keepdims=True)
    hi, lo = split(p)
    return jnp.concatenate([hi, lo], 0).T, jnp.concatenate([hi, ext_rows(bias, True)], 0).T


def body(t_hbm, g_hbm, w_hbm, out_ref, tbuf, sbuf, lhs, rhs, acc, part, got,
         loc_sem, ss, sr, ds, dr, ts, tr, ps, pr):
    me = coords()
    bar = pltpu.get_barrier_semaphore()
    peers = [(0, dx, dy, 0) for dx, dy in PLANE] + [(dz, 0, 0, 0) for dz in ZS] + [(0, 0, 0, 1)]
    for p in peers:
        pl.semaphore_signal(bar, 1, device_id=peer(me, *p), device_id_type=MESH)
    local = [
        pltpu.make_async_copy(g_hbm, sbuf.at[0, 0, pl.ds(0, D)], loc_sem.at[0]),
        pltpu.make_async_copy(w_hbm, sbuf.at[0, 0, pl.ds(D, 1)], loc_sem.at[1]),
        pltpu.make_async_copy(t_hbm, tbuf.at[0], loc_sem.at[2]),
    ]
    for c in local:
        c.start()
    acc[...] = jnp.zeros_like(acc)
    for c in local:
        c.wait()
    pl.semaphore_wait(bar, len(peers))

    def send(src, dst, s, r, **to):
        c = pltpu.make_async_remote_copy(src_ref=src, dst_ref=dst, send_sem=s, recv_sem=r, device_id=peer(me, **to), device_id_type=MESH)
        c.start()
        return c

    def rows(b, k):
        return sbuf.at[b, k, pl.ds(0, D + 1)]

    forward, sends = {}, {}
    forward[0] = send(rows(0, 0), rows(1, 0), ds.at[0], dr.at[0], dc=1)
    for dx, dy in ORDER[1:]:
        k = dx * 4 + dy
        sends[k] = send(rows(0, 0), rows(0, k), ss.at[k], sr.at[k], dx=dx, dy=dy)
    tsend = [send(tbuf.at[0], tbuf.at[i + 1], ts.at[i], tr.at[i], dz=dz) for i, dz in enumerate(ZS)]

    def prep_t(i):
        rhs[:, pl.ds(i * TGT, TGT)] = prep_targets(tbuf[i])

    def prep_s(b, k, at):
        a, e = prep_sources(sbuf[b, k, 0:D], sbuf[b, k, D:D + 1])
        lhs[pl.ds(at * SRC, SRC), 0:128] = a
        lhs[pl.ds(at * SRC, SRC), 128:256] = e

    def unit(group, i):
        n = 2 * PER * SRC
        x = jnp.dot(lhs[pl.ds(group * n, n), :], rhs[:, pl.ds(i * TGT, TGT)], preferred_element_type=f32)
        e = jnp.exp2(x)
        acc[:, pl.ds(i * TGT, TGT)] += e.reshape(n // 8, 8, TGT).sum(0)

    prep_t(0)
    for g in range(GROUPS):
        ks = [dx * 4 + dy for dx, dy in ORDER[g * PER:(g + 1) * PER]]
        for k in ks:
            if k:
                sends[k].wait_recv()
                forward[k] = send(rows(0, k), rows(1, k), ds.at[k], dr.at[k], dc=1)
        for j, k in enumerate(ks):
            prep_s(0, k, g * 2 * PER + 2 * j)
        for j, k in enumerate(ks):
            forward[k].wait_recv()
            prep_s(1, k, g * 2 * PER + 2 * j + 1)
        unit(g, 0)
    psend = []
    for i in range(len(ZS)):
        tsend[i].wait_recv()
        prep_t(i + 1)
        for g in range(GROUPS):
            unit(g, i + 1)
        v = jnp.sum(acc[:, pl.ds((i + 1) * TGT, TGT)], axis=0, keepdims=True)
        part[i, 0:1, :] = v
        psend.append(send(part.at[i], got.at[i], ps.at[i], pr.at[i], dz=4 - ZS[i]))
    total = jnp.sum(acc[:, pl.ds(0, TGT)], axis=0, keepdims=True)
    for c in psend:
        c.wait_recv()
    for i in range(len(ZS)):
        total = total + got[i, 0:1, :]
    out_ref[...] = total
    for c in list(sends.values()) + list(forward.values()) + tsend + psend:
        c.wait_send()


def shards(targets, source_grid, source_weight):
    any_spec = pl.BlockSpec(memory_space=pl.ANY)
    out = pl.pallas_call(
        body,
        out_shape=jax.ShapeDtypeStruct((1, TGT), f32),
        in_specs=[any_spec] * 3,
        out_specs=pl.BlockSpec(memory_space=pltpu.VMEM),
        scratch_shapes=[
            pltpu.VMEM((4, D, TGT), f32),
            pltpu.VMEM((2, 16, D + 8, SRC), i32),
            pltpu.VMEM((32 * SRC, 256), bf16),
            pltpu.VMEM((256, 4 * TGT), bf16),
            pltpu.VMEM((8, 4 * TGT), f32),
            pltpu.VMEM((3, 1, TGT), f32),
            pltpu.VMEM((3, 1, TGT), f32),
            DMA((3,)), DMA((16,)), DMA((16,)), DMA((16,)), DMA((16,)), DMA((3,)), DMA((3,)), DMA((3,)), DMA((3,)),
        ],
        compiler_params=pltpu.CompilerParams(collective_id=0, has_side_effects=True),
    )(targets, source_grid, source_weight)
    return out.reshape(TGT)


def solution(mesh):
    in_specs = (P(None, ("grp", "dev")), P(None, ("grp", "dev")), P(None, ("grp", "dev")))
    return jax.shard_map(shards, mesh=mesh, in_specs=in_specs, out_specs=P(("grp", "dev")), check_vma=False)
```

```python
import functools
import math

import jax
import jax.numpy as jnp
from jax import lax
from jax.experimental import pallas as pl
from jax.experimental.pallas import tpu as pltpu
from jax.sharding import PartitionSpec as P

KERNEL_RATE = 0.7
RATE2 = KERNEL_RATE * math.log2(math.e)
MESH = pl.DeviceIdType.MESH
DMA = pltpu.SemaphoreType.DMA
f32, bf16, i32 = jnp.float32, jnp.bfloat16, jnp.int32

D, TGT, SRC = 64, 512, 128
PLANE = [(dx, dy) for dx in range(4) for dy in range(4) if dx or dy]
ORDER = [(0, 0), (1, 0), (3, 0), (0, 1), (0, 3), (1, 1), (3, 1), (1, 3), (3, 3), (2, 0), (0, 2), (2, 1), (2, 3), (1, 2), (3, 2), (2, 2)]
ZS = (2, 1, 3)
ZS_ARRIVE = (1, 3, 2)
BOUNDS = (0, 4, 12, 16)
SLOTS = [0, 4, 12, 8, 1, 3, 2, 5, 7, 13, 15, 6, 14, 9, 11, 10]


def coords():
    g, d = lax.axis_index("grp"), lax.axis_index("dev")
    return lax.div(d, 8), lax.rem(lax.div(d, 2), 4), 2 * lax.rem(d, 2) + lax.div(g, 2), lax.rem(g, 2)


def peer(me, dz=0, dx=0, dy=0, dc=0):
    z, x, y, c = (lax.rem(a + b, n) for a, b, n in zip(me, (dz, dx, dy, dc), (4, 4, 4, 2)))
    return (lax.rem(y, 2) * 2 + c, z * 8 + x * 2 + lax.div(y, 2))


def ext_rows(v, first):
    a = v.astype(bf16).astype(f32)
    b = (v - a).astype(bf16).astype(f32)
    c = v - a - b
    row = lax.broadcasted_iota(i32, (8, v.shape[1]), 0)
    k, o = (0, 3) if first else (3, 0)
    ones = jnp.where((row >= o) & (row < o + 3), 1.0, 0.0)
    rows = jnp.where(row == k, a, jnp.where(row == k + 1, b, jnp.where(row == k + 2, c, ones)))
    return jnp.concatenate([rows, jnp.zeros((D - 8, v.shape[1]), f32)], 0).astype(bf16)


def split(v):
    hi = v.astype(bf16)
    return hi, (v - hi.astype(f32)).astype(bf16)


def prep_targets(t):
    norm = -RATE2 * jnp.sum(t * t, axis=0, keepdims=True)
    hi, lo = split(t * (2.0 * RATE2))
    return jnp.concatenate([hi, hi, lo, ext_rows(norm, False)], 0)


def prep_sources(grid, weight):
    p = grid.astype(f32) * (1.0 / 1048576.0)
    bias = jnp.log2(weight.astype(f32) * (1.0 / 16.0)) - RATE2 * jnp.sum(p * p, axis=0, keepdims=True)
    hi, lo = split(p)
    return jnp.concatenate([hi, lo], 0).T, jnp.concatenate([hi, ext_rows(bias, True)], 0).T


def body(t_hbm, g_hbm, w_hbm, out_ref, tbuf, sbuf, lhs, rhs, acc, part, got,
         loc_sem, ss, sr, ts, tr, fs, fr, ps, pr):
    me = coords()
    bar = pltpu.get_barrier_semaphore()
    peers = [(0, dx, dy, 0) for dx, dy in PLANE if not (dx and dy)] + [(dz, 0, 0, dc) for dz in range(4) for dc in range(2) if dz or dc]
    for p in peers:
        pl.semaphore_signal(bar, 1, device_id=peer(me, *p), device_id_type=MESH)
    local = [
        pltpu.make_async_copy(g_hbm, sbuf.at[0, pl.ds(0, D)], loc_sem.at[0]),
        pltpu.make_async_copy(w_hbm, sbuf.at[0, pl.ds(D, 1)], loc_sem.at[1]),
        pltpu.make_async_copy(t_hbm, tbuf.at[0], loc_sem.at[2]),
    ]
    for c in local:
        c.start()
    acc[...] = jnp.zeros_like(acc)
    for c in local:
        c.wait()
    pl.semaphore_wait(bar, len(peers))

    def send(src, dst, s, r, **to):
        c = pltpu.make_async_remote_copy(src_ref=src, dst_ref=dst, send_sem=s, recv_sem=r, device_id=peer(me, **to), device_id_type=MESH)
        c.start()
        return c

    def rows(k):
        return sbuf.at[k, pl.ds(0, D + 1)]

    sends, tsend, tfwd = {}, {}, {}
    c = me[3]

    def first(k):
        return dict(dx=k * (1 - c), dy=k * c)

    def second(k):
        return dict(dx=k * c, dy=k * (1 - c))

    def relay(k):
        for j in (2, 1, 3):
            n = 4 * k + j
            sends[n] = send(rows(4 * k), rows(n), ss.at[n], sr.at[n], **second(j))

    for k in (2, 1, 3):
        sends[4 * k] = send(rows(0), rows(4 * k), ss.at[4 * k], sr.at[4 * k], **first(k))
    relay(0)
    for dz in ZS:
        tsend[dz] = send(tbuf.at[0], tbuf.at[2 * dz], ts.at[dz], tr.at[dz], dz=dz)
    tfwd[0] = send(tbuf.at[0], tbuf.at[1], fs.at[0], fr.at[0], dc=1)

    def prep_t(i):
        rhs[:, pl.ds(i * TGT, TGT)] = prep_targets(tbuf[i])

    def prep_s(n):
        k = SLOTS[n]
        a, e = prep_sources(sbuf[k, 0:D], sbuf[k, D:D + 1])
        lhs[pl.ds(n * SRC, SRC), 0:128] = a
        lhs[pl.ds(n * SRC, SRC), 128:256] = e

    def lanes(i, w):
        return pl.ds(i * TGT if isinstance(i, int) else pl.multiple_of(i * TGT, TGT), w * TGT)

    def unit(g, i, w=2):
        n = (BOUNDS[g + 1] - BOUNDS[g]) * SRC
        x = jnp.dot(lhs[pl.ds(BOUNDS[g] * SRC, n), :], rhs[:, lanes(i, w)], preferred_element_type=f32)
        e = jnp.exp2(x)
        acc[:, lanes(i, w)] += e.reshape(n // 8, 8, w * TGT).sum(0)

    def group(g):
        for n in range(BOUNDS[g], BOUNDS[g + 1]):
            if SLOTS[n] % 4 or not n:
                if n:
                    sends[SLOTS[n]].wait_recv()
        for n in range(BOUNDS[g], BOUNDS[g + 1]):
            prep_s(n)

    def part_copy(i, dz, dc):
        return pltpu.make_async_remote_copy(src_ref=part.at[i], dst_ref=got.at[i], send_sem=ps.at[i], recv_sem=pr.at[i], device_id=peer(me, dz=dz, dc=dc), device_id_type=MESH)

    def reduce_part(i):
        part[i] = jnp.sum(acc[:, lanes(i, 1)], axis=0, keepdims=True)

    slots = []
    for u in range(3):
        zt = u + (u >= me[0]).astype(i32)
        slots.append(2 * lax.rem(me[0] - zt + 4, 4))

    prep_t(0)
    last = len(BOUNDS) - 2
    for k in (1, 3, 2):
        sends[4 * k].wait_recv()
        relay(k)
    group(0)
    unit(0, 0, 1)
    tfwd[0].wait_recv()
    prep_t(1)
    unit(0, 1, 1)
    for dz in ZS_ARRIVE:
        tsend[dz].wait_recv()
        tfwd[dz] = send(tbuf.at[2 * dz], tbuf.at[2 * dz + 1], fs.at[dz], fr.at[dz], dc=1)
        prep_t(2 * dz)
        unit(0, 2 * dz, 1)
    for dz in ZS_ARRIVE:
        tfwd[dz].wait_recv()
        prep_t(2 * dz + 1)
        unit(0, 2 * dz + 1, 1)
    for g in range(1, last):
        group(g)
        for i in (0, 2, 4, 6):
            unit(g, i)
    group(last)
    for i in slots:
        unit(last, i)
        reduce_part(i)
        reduce_part(i + 1)
        for dc in range(2):
            part_copy(i + dc, lax.rem(4 - lax.div(i, 2), 4), dc).start()
    unit(last, 0)
    reduce_part(1)
    part_copy(1, 0, 1).start()
    total = jnp.sum(acc[:, lanes(0, 1)], axis=0, keepdims=True)
    for i in range(1, 8):
        part_copy(i, 0, 1).wait_recv()
        total = total + got[i]
    out_ref[...] = total
    for c in list(sends.values()) + list(tsend.values()) + list(tfwd.values()):
        c.wait_send()
    for i in range(1, 8):
        part_copy(i, 0, 1).wait_send()


def shards(targets, source_grid, source_weight):
    any_spec = pl.BlockSpec(memory_space=pltpu.HBM)
    targets, source_grid, source_weight = (pltpu.with_memory_space_constraint(v, pltpu.HBM) for v in (targets, source_grid, source_weight))
    out = pl.pallas_call(
        body,
        out_shape=jax.ShapeDtypeStruct((1, TGT), f32),
        in_specs=[any_spec] * 3,
        out_specs=pl.BlockSpec(memory_space=pltpu.VMEM),
        scratch_shapes=[
            pltpu.VMEM((8, D, TGT), f32),
            pltpu.VMEM((16, D + 8, SRC), i32),
            pltpu.VMEM((16 * SRC, 256), bf16),
            pltpu.VMEM((256, 8 * TGT), bf16),
            pltpu.VMEM((8, 8 * TGT), f32),
            pltpu.VMEM((8, 1, TGT), f32),
            pltpu.VMEM((8, 1, TGT), f32),
            DMA((3,)), DMA((16,)), DMA((16,)), DMA((4,)), DMA((4,)), DMA((4,)), DMA((4,)), DMA((8,)), DMA((8,)),
        ],
        compiler_params=pltpu.CompilerParams(collective_id=0, has_side_effects=True, vmem_limit_bytes=24 * 1024 * 1024),
    )(targets, source_grid, source_weight)
    return out.reshape(TGT)


def solution(mesh):
    in_specs = (P(None, ("grp", "dev")), P(None, ("grp", "dev")), P(None, ("grp", "dev")))
    return jax.shard_map(shards, mesh=mesh, in_specs=in_specs, out_specs=P(("grp", "dev")), check_vma=False)
```

```python
import functools
import math

import jax
import jax.numpy as jnp
from jax import lax
from jax.experimental import pallas as pl
from jax.experimental.pallas import tpu as pltpu
from jax.sharding import PartitionSpec as P

KERNEL_RATE = 0.7
RATE2 = KERNEL_RATE * math.log2(math.e)
MESH = pl.DeviceIdType.MESH
DMA = pltpu.SemaphoreType.DMA
f32, bf16, i32 = jnp.float32, jnp.bfloat16, jnp.int32

D, TGT, SRC = 64, 512, 128
PLANE = [(dx, dy) for dx in range(4) for dy in range(4) if dx or dy]
ORDER = [(0, 0), (1, 0), (3, 0), (0, 1), (0, 3), (1, 1), (3, 1), (1, 3), (3, 3), (2, 0), (0, 2), (2, 1), (2, 3), (1, 2), (3, 2), (2, 2)]
ZS = (2, 1, 3)
ZS_ARRIVE = (1, 3, 2)
BOUNDS = (0, 7, 16)
SLOTS = [0, 4, 12, 8, 1, 3, 2, 5, 7, 13, 15, 6, 14, 9, 11, 10]


def coords():
    g, d = lax.axis_index("grp"), lax.axis_index("dev")
    return lax.div(d, 8), lax.rem(lax.div(d, 2), 4), 2 * lax.rem(d, 2) + lax.div(g, 2), lax.rem(g, 2)


def peer(me, dz=0, dx=0, dy=0, dc=0):
    z, x, y, c = (lax.rem(a + b, n) for a, b, n in zip(me, (dz, dx, dy, dc), (4, 4, 4, 2)))
    return (lax.rem(y, 2) * 2 + c, z * 8 + x * 2 + lax.div(y, 2))


def rank(v):
    return lax.select(v < 2, v, 5 - v)


def ext_rows(v, first):
    a = v.astype(bf16).astype(f32)
    b = (v - a).astype(bf16).astype(f32)
    c = v - a - b
    row = lax.broadcasted_iota(i32, (8, v.shape[1]), 0)
    k, o = (0, 3) if first else (3, 0)
    ones = jnp.where((row >= o) & (row < o + 3), 1.0, 0.0)
    rows = jnp.where(row == k, a, jnp.where(row == k + 1, b, jnp.where(row == k + 2, c, ones)))
    return jnp.concatenate([rows, jnp.zeros((D - 8, v.shape[1]), f32)], 0).astype(bf16)


def split(v):
    hi = v.astype(bf16)
    return hi, (v - hi.astype(f32)).astype(bf16)


def prep_targets(t):
    norm = -RATE2 * jnp.sum(t * t, axis=0, keepdims=True)
    hi, lo = split(t * (2.0 * RATE2))
    return jnp.concatenate([hi, hi, lo, ext_rows(norm, False)], 0)


def prep_sources(grid, weight):
    p = grid.astype(f32) * (1.0 / 1048576.0)
    bias = jnp.log2(weight.astype(f32) * (1.0 / 16.0)) - RATE2 * jnp.sum(p * p, axis=0, keepdims=True)
    hi, lo = split(p)
    return jnp.concatenate([hi, lo], 0).T, jnp.concatenate([hi, ext_rows(bias, True)], 0).T


def body(t_hbm, g_hbm, w_hbm, out_ref, tbuf, sbuf, lhs, rhs, acc, part, got,
         loc_sem, ss, sr, ts, tr, fs, fr, ps, pr, ready):
    me = coords()
    z, x, y, c = me
    bar = pltpu.get_barrier_semaphore()
    axes = ("dx", "dy", "dz")
    lower = {}
    for name, v in zip(axes, (x, y, z)):
        for k in (1, 3, 2):
            lower[name, k] = rank(lax.rem(v + k, 4)) < rank(v)
    for (name, k), low in lower.items():
        @pl.when(jnp.logical_not(low))
        def _():
            pl.semaphore_signal(bar, 1, device_id=peer(me, **{name: k}), device_id_type=MESH)

    @pl.when(c == 1)
    def _():
        pl.semaphore_signal(bar, 1, device_id=peer(me, dc=1), device_id_type=MESH)

    local = [
        pltpu.make_async_copy(g_hbm, sbuf.at[0, pl.ds(0, D)], loc_sem.at[0]),
        pltpu.make_async_copy(w_hbm, sbuf.at[0, pl.ds(D, 1)], loc_sem.at[1]),
        pltpu.make_async_copy(t_hbm, tbuf.at[0], loc_sem.at[2]),
    ]
    for cp in local:
        cp.start()
    acc[...] = jnp.zeros_like(acc)
    count = 1 - c
    for low in lower.values():
        count = count + low.astype(i32)

    @pl.when(count > 0)
    def _():
        pl.semaphore_wait(bar, count)

    for (name, k), low in lower.items():
        @pl.when(low)
        def _():
            pl.semaphore_signal(ready.at[axes.index(name), 4 - k], 1, device_id=peer(me, **{name: k}), device_id_type=MESH)

    @pl.when(c == 0)
    def _():
        pl.semaphore_signal(ready.at[0, 0], 1, device_id=peer(me, dc=1), device_id_type=MESH)

    for cp in local:
        cp.wait()

    def copy(src, dst, s, r, **to):
        return pltpu.make_async_remote_copy(src_ref=src, dst_ref=dst, send_sem=s, recv_sem=r, device_id=peer(me, **to), device_id_type=MESH)

    def send(*args, **to):
        cp = copy(*args, **to)
        cp.start()
        return cp

    def rows(k):
        return sbuf.at[k, pl.ds(0, D + 1)]

    sends, tsend, tfwd = {}, {}, {}

    def first(k):
        return dict(dx=k * (1 - c), dy=k * c)

    def second(k):
        return dict(dx=k * c, dy=k * (1 - c))

    def relay(k):
        for j in (2, 1, 3):
            n = 4 * k + j
            sends[n] = send(rows(4 * k), rows(n), ss.at[n], sr.at[n], **second(j))

    opening = []
    for k in (1, 3, 2):
        lx, ly = lower["dx", k], lower["dy", k]
        sends[4 * k] = copy(rows(0), rows(4 * k), ss.at[4 * k], sr.at[4 * k], **first(k))
        sends[k] = copy(rows(0), rows(k), ss.at[k], sr.at[k], **second(k))
        tsend[k] = copy(tbuf.at[0], tbuf.at[2 * k], ts.at[k], tr.at[k], dz=k)
        opening.append((0, sends[4 * k], jnp.logical_or(jnp.logical_and(c == 0, lx), jnp.logical_and(c == 1, ly)), ready.at[c, k]))
        opening.append((0, sends[k], jnp.logical_or(jnp.logical_and(c == 1, lx), jnp.logical_and(c == 0, ly)), ready.at[1 - c, k]))
        opening.append((1, tsend[k], lower["dz", k], ready.at[2, k]))
    opening.sort(key=lambda o: o[0])
    for _, cp, low, _ in opening:
        @pl.when(low)
        def _():
            cp.start()

    @pl.when(c == 1)
    def _():
        pl.semaphore_wait(ready.at[0, 0], 1)

    tfwd[0] = send(tbuf.at[0], tbuf.at[1], fs.at[0], fr.at[0], dc=1)
    for _, cp, low, sem in opening:
        @pl.when(jnp.logical_not(low))
        def _():
            pl.semaphore_wait(sem, 1)
            cp.start()

    def prep_t(i):
        rhs[:, pl.ds(i * TGT, TGT)] = prep_targets(tbuf[i])

    def prep_s(n):
        k = SLOTS[n]
        a, e = prep_sources(sbuf[k, 0:D], sbuf[k, D:D + 1])
        lhs[pl.ds(n * SRC, SRC), 0:128] = a
        lhs[pl.ds(n * SRC, SRC), 128:256] = e

    def lanes(i, w):
        return pl.ds(i * TGT if isinstance(i, int) else pl.multiple_of(i * TGT, TGT), w * TGT)

    def unit(g, i, w=2):
        n = (BOUNDS[g + 1] - BOUNDS[g]) * SRC
        x = jnp.dot(lhs[pl.ds(BOUNDS[g] * SRC, n), :], rhs[:, lanes(i, w)], preferred_element_type=f32)
        e = jnp.exp2(x)
        acc[:, lanes(i, w)] += e.reshape(n // 8, 8, w * TGT).sum(0)

    def group(g):
        for n in range(BOUNDS[g], BOUNDS[g + 1]):
            if SLOTS[n] % 4 or not n:
                if n:
                    sends[SLOTS[n]].wait_recv()
        for n in range(BOUNDS[g], BOUNDS[g + 1]):
            prep_s(n)

    def part_copy(i, dz, dc):
        return pltpu.make_async_remote_copy(src_ref=part.at[i], dst_ref=got.at[i], send_sem=ps.at[i], recv_sem=pr.at[i], device_id=peer(me, dz=dz, dc=dc), device_id_type=MESH)

    def reduce_part(i):
        part[i] = jnp.sum(acc[:, lanes(i, 1)], axis=0, keepdims=True)

    slots = []
    for u in range(3):
        zt = u + (u >= me[0]).astype(i32)
        slots.append(2 * lax.rem(me[0] - zt + 4, 4))

    prep_t(0)
    last = len(BOUNDS) - 2
    for k in (1, 3, 2):
        sends[4 * k].wait_recv()
        relay(k)
    group(0)
    unit(0, 0, 1)
    tfwd[0].wait_recv()
    prep_t(1)
    unit(0, 1, 1)
    for dz in ZS_ARRIVE:
        tsend[dz].wait_recv()
        tfwd[dz] = send(tbuf.at[2 * dz], tbuf.at[2 * dz + 1], fs.at[dz], fr.at[dz], dc=1)
        prep_t(2 * dz)
        unit(0, 2 * dz, 1)
    for dz in ZS_ARRIVE:
        tfwd[dz].wait_recv()
        prep_t(2 * dz + 1)
        unit(0, 2 * dz + 1, 1)
    for g in range(1, last):
        group(g)
        for i in (0, 2, 4, 6):
            unit(g, i)
    group(last)
    for i in slots:
        unit(last, i)
        reduce_part(i)
        reduce_part(i + 1)
        for dc in range(2):
            part_copy(i + dc, lax.rem(4 - lax.div(i, 2), 4), dc).start()
    unit(last, 0)
    reduce_part(1)
    part_copy(1, 0, 1).start()
    total = jnp.sum(acc[:, lanes(0, 1)], axis=0, keepdims=True)
    for i in range(1, 8):
        part_copy(i, 0, 1).wait_recv()
        total = total + got[i]
    out_ref[...] = total
    for c in list(sends.values()) + list(tsend.values()) + list(tfwd.values()):
        c.wait_send()
    for i in range(1, 8):
        part_copy(i, 0, 1).wait_send()


def shards(targets, source_grid, source_weight):
    any_spec = pl.BlockSpec(memory_space=pltpu.HBM)
    targets, source_grid, source_weight = (pltpu.with_memory_space_constraint(v, pltpu.HBM) for v in (targets, source_grid, source_weight))
    out = pl.pallas_call(
        body,
        out_shape=jax.ShapeDtypeStruct((1, TGT), f32),
        in_specs=[any_spec] * 3,
        out_specs=pl.BlockSpec(memory_space=pltpu.VMEM),
        scratch_shapes=[
            pltpu.VMEM((8, D, TGT), f32),
            pltpu.VMEM((16, D + 8, SRC), i32),
            pltpu.VMEM((16 * SRC, 256), bf16),
            pltpu.VMEM((256, 8 * TGT), bf16),
            pltpu.VMEM((8, 8 * TGT), f32),
            pltpu.VMEM((8, 1, TGT), f32),
            pltpu.VMEM((8, 1, TGT), f32),
            DMA((3,)), DMA((16,)), DMA((16,)), DMA((4,)), DMA((4,)), DMA((4,)), DMA((4,)), DMA((8,)), DMA((8,)), pltpu.SemaphoreType.REGULAR((3, 4)),
        ],
        compiler_params=pltpu.CompilerParams(collective_id=0, has_side_effects=True, vmem_limit_bytes=24 * 1024 * 1024),
    )(targets, source_grid, source_weight)
    return out.reshape(TGT)


def solution(mesh):
    in_specs = (P(None, ("grp", "dev")), P(None, ("grp", "dev")), P(None, ("grp", "dev")))
    return jax.shard_map(shards, mesh=mesh, in_specs=in_specs, out_specs=P(("grp", "dev")), check_vma=False)
```

```python
import functools
import math

import jax
import jax.numpy as jnp
from jax import lax
from jax.experimental import pallas as pl
from jax.experimental.pallas import tpu as pltpu
from jax.sharding import PartitionSpec as P

KERNEL_RATE = 0.7
RATE2 = KERNEL_RATE * math.log2(math.e)
MESH = pl.DeviceIdType.MESH
DMA = pltpu.SemaphoreType.DMA
f32, bf16, i32 = jnp.float32, jnp.bfloat16, jnp.int32

D, TGT, SRC = 64, 512, 128
PLANE = [(dx, dy) for dx in range(4) for dy in range(4) if dx or dy]
ORDER = [(0, 0), (1, 0), (3, 0), (0, 1), (0, 3), (1, 1), (3, 1), (1, 3), (3, 3), (2, 0), (0, 2), (2, 1), (2, 3), (1, 2), (3, 2), (2, 2)]
ZS = (2, 1, 3)
ZS_ARRIVE = (1, 3, 2)
EARLY, LATE = 4, ((4, 11), (11, 16))
SLOTS = [0, 4, 12, 8, 1, 3, 2, 5, 7, 13, 15, 6, 14, 9, 11, 10]


def coords():
    g, d = lax.axis_index("grp"), lax.axis_index("dev")
    return lax.div(d, 8), lax.rem(lax.div(d, 2), 4), 2 * lax.rem(d, 2) + lax.div(g, 2), lax.rem(g, 2)


def peer(me, dz=0, dx=0, dy=0, dc=0):
    z, x, y, c = (lax.rem(a + b, n) for a, b, n in zip(me, (dz, dx, dy, dc), (4, 4, 4, 2)))
    return (lax.rem(y, 2) * 2 + c, z * 8 + x * 2 + lax.div(y, 2))


def rank(v):
    return lax.select(v < 2, v, 5 - v)


def ext_rows(v, first):
    a = v.astype(bf16).astype(f32)
    b = (v - a).astype(bf16).astype(f32)
    c = v - a - b
    row = lax.broadcasted_iota(i32, (8, v.shape[1]), 0)
    k, o = (0, 3) if first else (3, 0)
    ones = jnp.where((row >= o) & (row < o + 3), 1.0, 0.0)
    rows = jnp.where(row == k, a, jnp.where(row == k + 1, b, jnp.where(row == k + 2, c, ones)))
    return jnp.concatenate([rows, jnp.zeros((D - 8, v.shape[1]), f32)], 0).astype(bf16)


def split(v):
    hi = v.astype(bf16)
    return hi, (v - hi.astype(f32)).astype(bf16)


def prep_targets(t):
    norm = -RATE2 * jnp.sum(t * t, axis=0, keepdims=True)
    hi, lo = split(t * (2.0 * RATE2))
    return jnp.concatenate([hi, hi, lo, ext_rows(norm, False)], 0)


def prep_sources(grid, weight):
    p = grid.astype(f32) * (1.0 / 1048576.0)
    bias = jnp.log2(weight.astype(f32) * (1.0 / 16.0)) - RATE2 * jnp.sum(p * p, axis=0, keepdims=True)
    hi, lo = split(p)
    return jnp.concatenate([hi, lo], 0).T, jnp.concatenate([hi, ext_rows(bias, True)], 0).T


def body(t_hbm, g_hbm, w_hbm, out_ref, tbuf, sbuf, lhs, rhs, acc, part, got,
         loc_sem, ss, sr, ts, tr, fs, fr, ps, pr, ready):
    me = coords()
    z, x, y, c = me
    local = [
        pltpu.make_async_copy(g_hbm, sbuf.at[0, pl.ds(0, D)], loc_sem.at[0]),
        pltpu.make_async_copy(w_hbm, sbuf.at[0, pl.ds(D, 1)], loc_sem.at[1]),
        pltpu.make_async_copy(t_hbm, tbuf.at[0], loc_sem.at[2]),
    ]
    for cp in local:
        cp.start()
    bar = pltpu.get_barrier_semaphore()
    axes = ("dx", "dy", "dz")
    lower = {}
    for name, v in zip(axes, (x, y, z)):
        for k in (1, 3, 2):
            lower[name, k] = rank(lax.rem(v + k, 4)) < rank(v)
    for (name, k), low in lower.items():
        @pl.when(jnp.logical_not(low))
        def _():
            pl.semaphore_signal(bar, 1, device_id=peer(me, **{name: k}), device_id_type=MESH)

    @pl.when(c == 1)
    def _():
        pl.semaphore_signal(bar, 1, device_id=peer(me, dc=1), device_id_type=MESH)

    acc[...] = jnp.zeros_like(acc)
    count = 1 - c
    for low in lower.values():
        count = count + low.astype(i32)

    @pl.when(count > 0)
    def _():
        pl.semaphore_wait(bar, count)

    for (name, k), low in lower.items():
        @pl.when(low)
        def _():
            pl.semaphore_signal(ready.at[axes.index(name), 4 - k], 1, device_id=peer(me, **{name: k}), device_id_type=MESH)

    @pl.when(c == 0)
    def _():
        pl.semaphore_signal(ready.at[0, 0], 1, device_id=peer(me, dc=1), device_id_type=MESH)

    for cp in local:
        cp.wait()

    def copy(src, dst, s, r, **to):
        return pltpu.make_async_remote_copy(src_ref=src, dst_ref=dst, send_sem=s, recv_sem=r, device_id=peer(me, **to), device_id_type=MESH)

    def send(*args, **to):
        cp = copy(*args, **to)
        cp.start()
        return cp

    def rows(k):
        return sbuf.at[k, pl.ds(0, D + 1)]

    sends, tsend, tfwd = {}, {}, {}

    def first(k):
        return dict(dx=k * (1 - c), dy=k * c)

    def second(k):
        return dict(dx=k * c, dy=k * (1 - c))

    def relay(k):
        for j in (2, 1, 3):
            n = 4 * k + j
            sends[n] = send(rows(4 * k), rows(n), ss.at[n], sr.at[n], **second(j))

    opening = []
    for k in (1, 3, 2):
        lx, ly = lower["dx", k], lower["dy", k]
        sends[4 * k] = copy(rows(0), rows(4 * k), ss.at[4 * k], sr.at[4 * k], **first(k))
        sends[k] = copy(rows(0), rows(k), ss.at[k], sr.at[k], **second(k))
        tsend[k] = copy(tbuf.at[0], tbuf.at[2 * k], ts.at[k], tr.at[k], dz=k)
        opening.append((0, sends[4 * k], jnp.logical_or(jnp.logical_and(c == 0, lx), jnp.logical_and(c == 1, ly)), ready.at[c, k]))
        opening.append((0, sends[k], jnp.logical_or(jnp.logical_and(c == 1, lx), jnp.logical_and(c == 0, ly)), ready.at[1 - c, k]))
        opening.append((1, tsend[k], lower["dz", k], ready.at[2, k]))
    opening.sort(key=lambda o: o[0])
    for _, cp, low, _ in opening:
        @pl.when(low)
        def _():
            cp.start()

    @pl.when(c == 1)
    def _():
        pl.semaphore_wait(ready.at[0, 0], 1)

    tfwd[0] = send(tbuf.at[0], tbuf.at[1], fs.at[0], fr.at[0], dc=1)
    for _, cp, low, sem in opening:
        @pl.when(jnp.logical_not(low))
        def _():
            pl.semaphore_wait(sem, 1)
            cp.start()

    def prep_t(i):
        rhs[:, pl.ds(i * TGT, TGT)] = prep_targets(tbuf[i])

    def prep_s(n):
        k = SLOTS[n]
        a, e = prep_sources(sbuf[k, 0:D], sbuf[k, D:D + 1])
        lhs[pl.ds(n * SRC, SRC), 0:128] = a
        lhs[pl.ds(n * SRC, SRC), 128:256] = e

    def lanes(i, w):
        return pl.ds(i * TGT if isinstance(i, int) else pl.multiple_of(i * TGT, TGT), w * TGT)

    def unit(lo, hi, i, w=2):
        n = (hi - lo) * SRC
        x = jnp.dot(lhs[pl.ds(lo * SRC, n), :], rhs[:, lanes(i, w)], preferred_element_type=f32)
        e = jnp.exp2(x)
        acc[:, lanes(i, w)] += e.reshape(n // 8, 8, w * TGT).sum(0)

    def group(lo, hi):
        for n in range(lo, hi):
            if SLOTS[n] % 4:
                sends[SLOTS[n]].wait_recv()
        for n in range(lo, hi):
            prep_s(n)

    def part_copy(i, dz, dc):
        return pltpu.make_async_remote_copy(src_ref=part.at[i], dst_ref=got.at[i], send_sem=ps.at[i], recv_sem=pr.at[i], device_id=peer(me, dz=dz, dc=dc), device_id_type=MESH)

    def reduce_part(i):
        part[i] = jnp.sum(acc[:, lanes(i, 1)], axis=0, keepdims=True)

    slots = []
    for u in range(3):
        zt = u + (u >= me[0]).astype(i32)
        slots.append(2 * lax.rem(me[0] - zt + 4, 4))

    prep_t(0)
    for k in (1, 3, 2):
        sends[4 * k].wait_recv()
        relay(k)
    group(0, EARLY)
    unit(0, EARLY, 0, 1)
    tfwd[0].wait_recv()
    prep_t(1)
    unit(0, EARLY, 1, 1)
    for dz in ZS_ARRIVE:
        tsend[dz].wait_recv()
        tfwd[dz] = send(tbuf.at[2 * dz], tbuf.at[2 * dz + 1], fs.at[dz], fr.at[dz], dc=1)
        prep_t(2 * dz)
        unit(0, EARLY, 2 * dz, 1)
    for dz in ZS_ARRIVE:
        tfwd[dz].wait_recv()
        prep_t(2 * dz + 1)
        unit(0, EARLY, 2 * dz + 1, 1)
    for lo, hi in LATE:
        group(lo, hi)
        unit(lo, hi, slots[0])
    for u, i in enumerate(slots):
        if u:
            unit(EARLY, 16, i)
        reduce_part(i)
        reduce_part(i + 1)
        for dc in range(2):
            part_copy(i + dc, lax.rem(4 - lax.div(i, 2), 4), dc).start()
    unit(EARLY, 16, 0)
    reduce_part(1)
    part_copy(1, 0, 1).start()
    for cp in list(sends.values()) + list(tsend.values()) + list(tfwd.values()):
        cp.wait_send()
    total = jnp.sum(acc[:, lanes(0, 1)], axis=0, keepdims=True)
    for i in range(1, 8):
        part_copy(i, 0, 1).wait_send()
    for i in range(1, 8):
        part_copy(i, 0, 1).wait_recv()
        total = total + got[i]
    out_ref[...] = total


def shards(targets, source_grid, source_weight):
    any_spec = pl.BlockSpec(memory_space=pltpu.HBM)
    targets, source_grid, source_weight = (pltpu.with_memory_space_constraint(v, pltpu.HBM) for v in (targets, source_grid, source_weight))
    out = pl.pallas_call(
        body,
        out_shape=jax.ShapeDtypeStruct((1, TGT), f32),
        in_specs=[any_spec] * 3,
        out_specs=pl.BlockSpec(memory_space=pltpu.VMEM),
        scratch_shapes=[
            pltpu.VMEM((8, D, TGT), f32),
            pltpu.VMEM((16, D + 8, SRC), i32),
            pltpu.VMEM((16 * SRC, 256), bf16),
            pltpu.VMEM((256, 8 * TGT), bf16),
            pltpu.VMEM((8, 8 * TGT), f32),
            pltpu.VMEM((8, 1, TGT), f32),
            pltpu.VMEM((8, 1, TGT), f32),
            DMA((3,)), DMA((16,)), DMA((16,)), DMA((4,)), DMA((4,)), DMA((4,)), DMA((4,)), DMA((8,)), DMA((8,)), pltpu.SemaphoreType.REGULAR((3, 4)),
        ],
        compiler_params=pltpu.CompilerParams(collective_id=0, has_side_effects=True, vmem_limit_bytes=24 * 1024 * 1024),
    )(targets, source_grid, source_weight)
    return out.reshape(TGT)


def solution(mesh):
    in_specs = (P(None, ("grp", "dev")), P(None, ("grp", "dev")), P(None, ("grp", "dev")))
    return jax.shard_map(shards, mesh=mesh, in_specs=in_specs, out_specs=P(("grp", "dev")), check_vma=False)
```

```python
import functools
import math

import jax
import jax.numpy as jnp
from jax import lax
from jax.experimental import pallas as pl
from jax.experimental.pallas import tpu as pltpu
from jax.sharding import PartitionSpec as P

KERNEL_RATE = 0.7
RATE2 = KERNEL_RATE * math.log2(math.e)
MESH = pl.DeviceIdType.MESH
DMA = pltpu.SemaphoreType.DMA
f32, bf16, i32 = jnp.float32, jnp.bfloat16, jnp.int32

D, TGT, SRC = 64, 512, 128
PLANE = [(dx, dy) for dx in range(4) for dy in range(4) if dx or dy]
ORDER = [(0, 0), (1, 0), (3, 0), (0, 1), (0, 3), (1, 1), (3, 1), (1, 3), (3, 3), (2, 0), (0, 2), (2, 1), (2, 3), (1, 2), (3, 2), (2, 2)]
ZS = (2, 1, 3)
ZS_ARRIVE = (1, 3, 2)
EARLY, LATE = 4, ((4, 11), (11, 16))
SLOTS = [0, 4, 12, 8, 1, 3, 2, 5, 7, 13, 15, 6, 14, 9, 11, 10]


def coords():
    g, d = lax.axis_index("grp"), lax.axis_index("dev")
    return lax.div(d, 8), lax.rem(lax.div(d, 2), 4), 2 * lax.rem(d, 2) + lax.div(g, 2), lax.rem(g, 2)


def peer(me, dz=0, dx=0, dy=0, dc=0):
    z, x, y, c = (lax.rem(a + b, n) for a, b, n in zip(me, (dz, dx, dy, dc), (4, 4, 4, 2)))
    return (lax.rem(y, 2) * 2 + c, z * 8 + x * 2 + lax.div(y, 2))


def rank(v):
    return lax.select(v < 2, v, 5 - v)


def ext_rows(v, first):
    a = v.astype(bf16).astype(f32)
    b = (v - a).astype(bf16).astype(f32)
    c = v - a - b
    row = lax.broadcasted_iota(i32, (8, v.shape[1]), 0)
    k, o = (0, 3) if first else (3, 0)
    ones = jnp.where((row >= o) & (row < o + 3), 1.0, 0.0)
    rows = jnp.where(row == k, a, jnp.where(row == k + 1, b, jnp.where(row == k + 2, c, ones)))
    return jnp.concatenate([rows, jnp.zeros((D - 8, v.shape[1]), f32)], 0).astype(bf16)


def split(v):
    hi = v.astype(bf16)
    return hi, (v - hi.astype(f32)).astype(bf16)


def prep_targets(t):
    norm = -RATE2 * jnp.sum(t * t, axis=0, keepdims=True)
    hi, lo = split(t * (2.0 * RATE2))
    return jnp.concatenate([hi, hi, lo, ext_rows(norm, False)], 0)


def prep_sources(grid, weight):
    p = grid.astype(f32) * (1.0 / 1048576.0)
    bias = jnp.log2(weight.astype(f32) * (1.0 / 16.0)) - RATE2 * jnp.sum(p * p, axis=0, keepdims=True)
    hi, lo = split(p)
    return jnp.concatenate([hi, lo], 0).T, jnp.concatenate([hi, ext_rows(bias, True)], 0).T


def body(t_hbm, g_hbm, w_hbm, out_ref, tbuf, sbuf, lhs, rhs, acc, part, got,
         loc_sem, ss, sr, ts, tr, fs, fr, ps, pr, ready):
    me = coords()
    z, x, y, c = me
    local = [
        pltpu.make_async_copy(g_hbm, sbuf.at[0, pl.ds(0, D)], loc_sem.at[0]),
        pltpu.make_async_copy(w_hbm, sbuf.at[0, pl.ds(D, 1)], loc_sem.at[1]),
        pltpu.make_async_copy(t_hbm, tbuf.at[0], loc_sem.at[2]),
    ]
    for cp in local:
        cp.start()
    bar = pltpu.get_barrier_semaphore()
    axes = ("dx", "dy", "dz")
    lower = {}
    for name, v in zip(axes, (x, y, z)):
        for k in (1, 3, 2):
            lower[name, k] = lax.rem(v + k, 4) < v if name == "dz" else rank(lax.rem(v + k, 4)) < rank(v)
    for (name, k), low in lower.items():
        @pl.when(jnp.logical_not(low))
        def _():
            pl.semaphore_signal(bar, 1, device_id=peer(me, **{name: k}), device_id_type=MESH)

    @pl.when(c == 1)
    def _():
        pl.semaphore_signal(bar, 1, device_id=peer(me, dc=1), device_id_type=MESH)

    acc[...] = jnp.zeros_like(acc)
    count = 1 - c
    for low in lower.values():
        count = count + low.astype(i32)

    @pl.when(count > 0)
    def _():
        pl.semaphore_wait(bar, count)

    for (name, k), low in lower.items():
        @pl.when(low)
        def _():
            pl.semaphore_signal(ready.at[axes.index(name), 4 - k], 1, device_id=peer(me, **{name: k}), device_id_type=MESH)

    @pl.when(c == 0)
    def _():
        pl.semaphore_signal(ready.at[0, 0], 1, device_id=peer(me, dc=1), device_id_type=MESH)

    for cp in local:
        cp.wait()

    def copy(src, dst, s, r, **to):
        return pltpu.make_async_remote_copy(src_ref=src, dst_ref=dst, send_sem=s, recv_sem=r, device_id=peer(me, **to), device_id_type=MESH)

    def send(*args, **to):
        cp = copy(*args, **to)
        cp.start()
        return cp

    def rows(k):
        return sbuf.at[k, pl.ds(0, D + 1)]

    sends, tsend, tfwd = {}, {}, {}

    def first(k):
        return dict(dx=k * (1 - c), dy=k * c)

    def second(k):
        return dict(dx=k * c, dy=k * (1 - c))

    def relay(k):
        for j in (2, 1, 3):
            n = 4 * k + j
            sends[n] = send(rows(4 * k), rows(n), ss.at[n], sr.at[n], **second(j))

    opening = []
    for k in (1, 3, 2):
        lx, ly = lower["dx", k], lower["dy", k]
        sends[4 * k] = copy(rows(0), rows(4 * k), ss.at[4 * k], sr.at[4 * k], **first(k))
        sends[k] = copy(rows(0), rows(k), ss.at[k], sr.at[k], **second(k))
        tsend[k] = copy(tbuf.at[0], tbuf.at[2 * k], ts.at[k], tr.at[k], dz=k)
        opening.append((0, sends[4 * k], jnp.logical_or(jnp.logical_and(c == 0, lx), jnp.logical_and(c == 1, ly)), ready.at[c, k]))
        opening.append((0, sends[k], jnp.logical_or(jnp.logical_and(c == 1, lx), jnp.logical_and(c == 0, ly)), ready.at[1 - c, k]))
        opening.append((1, tsend[k], lower["dz", k], ready.at[2, k]))
    opening.sort(key=lambda o: o[0])
    for _, cp, low, _ in opening:
        @pl.when(low)
        def _():
            cp.start()

    @pl.when(c == 1)
    def _():
        pl.semaphore_wait(ready.at[0, 0], 1)

    tfwd[0] = send(tbuf.at[0], tbuf.at[1], fs.at[0], fr.at[0], dc=1)
    for _, cp, low, sem in opening:
        @pl.when(jnp.logical_not(low))
        def _():
            pl.semaphore_wait(sem, 1)
            cp.start()

    def prep_t(i):
        rhs[:, pl.ds(i * TGT, TGT)] = prep_targets(tbuf[i])

    def prep_s(n):
        k = SLOTS[n]
        a, e = prep_sources(sbuf[k, 0:D], sbuf[k, D:D + 1])
        lhs[pl.ds(n * SRC, SRC), 0:128] = a
        lhs[pl.ds(n * SRC, SRC), 128:256] = e

    def lanes(i, w):
        return pl.ds(i * TGT if isinstance(i, int) else pl.multiple_of(i * TGT, TGT), w * TGT)

    def unit(lo, hi, i, w=2):
        n = (hi - lo) * SRC
        x = jnp.dot(lhs[pl.ds(lo * SRC, n), :], rhs[:, lanes(i, w)], preferred_element_type=f32)
        e = jnp.exp2(x)
        acc[:, lanes(i, w)] += e.reshape(n // 8, 8, w * TGT).sum(0)

    def group(lo, hi):
        for n in range(lo, hi):
            if SLOTS[n] % 4:
                sends[SLOTS[n]].wait_recv()
        for n in range(lo, hi):
            prep_s(n)

    def part_copy(i, dz, dc):
        return pltpu.make_async_remote_copy(src_ref=part.at[i], dst_ref=got.at[i], send_sem=ps.at[i], recv_sem=pr.at[i], device_id=peer(me, dz=dz, dc=dc), device_id_type=MESH)

    def reduce_part(i):
        part[i] = jnp.sum(acc[:, lanes(i, 1)], axis=0, keepdims=True)

    slots = []
    for u in range(3):
        zt = u + (u >= me[0]).astype(i32)
        slots.append(2 * lax.rem(me[0] - zt + 4, 4))

    prep_t(0)
    for k in (1, 3, 2):
        sends[4 * k].wait_recv()
        relay(k)
    group(0, EARLY)
    unit(0, EARLY, 0, 1)
    tfwd[0].wait_recv()
    prep_t(1)
    unit(0, EARLY, 1, 1)
    for dz in ZS_ARRIVE:
        tsend[dz].wait_recv()
        tfwd[dz] = send(tbuf.at[2 * dz], tbuf.at[2 * dz + 1], fs.at[dz], fr.at[dz], dc=1)
        prep_t(2 * dz)
        unit(0, EARLY, 2 * dz, 1)
    for dz in ZS_ARRIVE:
        tfwd[dz].wait_recv()
        prep_t(2 * dz + 1)
        unit(0, EARLY, 2 * dz + 1, 1)
    for lo, hi in LATE:
        group(lo, hi)
        unit(lo, hi, slots[0])
    for u, i in enumerate(slots):
        if u:
            unit(EARLY, 16, i)
        reduce_part(i)
        reduce_part(i + 1)
        for dc in range(2):
            part_copy(i + dc, lax.rem(4 - lax.div(i, 2), 4), dc).start()
    unit(EARLY, 16, 0)
    reduce_part(1)
    part_copy(1, 0, 1).start()
    for cp in list(sends.values()) + list(tsend.values()) + list(tfwd.values()):
        cp.wait_send()
    total = jnp.sum(acc[:, lanes(0, 1)], axis=0, keepdims=True)
    for i in range(1, 8):
        part_copy(i, 0, 1).wait_send()
    for i in range(1, 8):
        part_copy(i, 0, 1).wait_recv()
        total = total + got[i]
    out_ref[...] = total


def shards(targets, source_grid, source_weight):
    any_spec = pl.BlockSpec(memory_space=pltpu.HBM)
    targets, source_grid, source_weight = (pltpu.with_memory_space_constraint(v, pltpu.HBM) for v in (targets, source_grid, source_weight))
    out = pl.pallas_call(
        body,
        out_shape=jax.ShapeDtypeStruct((1, TGT), f32),
        in_specs=[any_spec] * 3,
        out_specs=pl.BlockSpec(memory_space=pltpu.VMEM),
        scratch_shapes=[
            pltpu.VMEM((8, D, TGT), f32),
            pltpu.VMEM((16, D + 8, SRC), i32),
            pltpu.VMEM((16 * SRC, 256), bf16),
            pltpu.VMEM((256, 8 * TGT), bf16),
            pltpu.VMEM((8, 8 * TGT), f32),
            pltpu.VMEM((8, 1, TGT), f32),
            pltpu.VMEM((8, 1, TGT), f32),
            DMA((3,)), DMA((16,)), DMA((16,)), DMA((4,)), DMA((4,)), DMA((4,)), DMA((4,)), DMA((8,)), DMA((8,)), pltpu.SemaphoreType.REGULAR((3, 4)),
        ],
        compiler_params=pltpu.CompilerParams(collective_id=0, has_side_effects=True, vmem_limit_bytes=24 * 1024 * 1024),
    )(targets, source_grid, source_weight)
    return out.reshape(TGT)


def solution(mesh):
    in_specs = (P(None, ("grp", "dev")), P(None, ("grp", "dev")), P(None, ("grp", "dev")))
    return jax.shard_map(shards, mesh=mesh, in_specs=in_specs, out_specs=P(("grp", "dev")), check_vma=False)
```

```python
import functools
import math

import jax
import jax.numpy as jnp
from jax import lax
from jax.experimental import pallas as pl
from jax.experimental.pallas import tpu as pltpu
from jax.sharding import PartitionSpec as P

KERNEL_RATE = 0.7
RATE2 = KERNEL_RATE * math.log2(math.e)
MESH = pl.DeviceIdType.MESH
DMA = pltpu.SemaphoreType.DMA
f32, bf16, i32 = jnp.float32, jnp.bfloat16, jnp.int32

D, TGT, SRC = 64, 512, 128
PLANE = [(dx, dy) for dx in range(4) for dy in range(4) if dx or dy]
ORDER = [(0, 0), (1, 0), (3, 0), (0, 1), (0, 3), (1, 1), (3, 1), (1, 3), (3, 3), (2, 0), (0, 2), (2, 1), (2, 3), (1, 2), (3, 2), (2, 2)]
ZS = (2, 1, 3)
ZS_ARRIVE = (3, 1, 2)
EARLY, LATE = 4, ((4, 11), (11, 16))
SLOTS = [0, 4, 12, 8, 1, 3, 2, 5, 7, 13, 15, 6, 14, 9, 11, 10]


def coords():
    g, d = lax.axis_index("grp"), lax.axis_index("dev")
    return lax.div(d, 8), lax.rem(lax.div(d, 2), 4), 2 * lax.rem(d, 2) + lax.div(g, 2), lax.rem(g, 2)


def peer(me, dz=0, dx=0, dy=0, dc=0):
    z, x, y, c = (lax.rem(a + b, n) for a, b, n in zip(me, (dz, dx, dy, dc), (4, 4, 4, 2)))
    return (lax.rem(y, 2) * 2 + c, z * 8 + x * 2 + lax.div(y, 2))


def rank(v):
    return lax.select(v < 2, v, 5 - v)


def ext_rows(v, first):
    a = v.astype(bf16).astype(f32)
    b = (v - a).astype(bf16).astype(f32)
    c = v - a - b
    row = lax.broadcasted_iota(i32, (8, v.shape[1]), 0)
    k, o = (0, 3) if first else (3, 0)
    ones = jnp.where((row >= o) & (row < o + 3), 1.0, 0.0)
    rows = jnp.where(row == k, a, jnp.where(row == k + 1, b, jnp.where(row == k + 2, c, ones)))
    return jnp.concatenate([rows, jnp.zeros((D - 8, v.shape[1]), f32)], 0).astype(bf16)


def split(v):
    hi = v.astype(bf16)
    return hi, (v - hi.astype(f32)).astype(bf16)


def prep_targets(t):
    norm = -RATE2 * jnp.sum(t * t, axis=0, keepdims=True)
    hi, lo = split(t * (2.0 * RATE2))
    return jnp.concatenate([hi, hi, lo, ext_rows(norm, False)], 0)


def prep_sources(grid, weight):
    p = grid.astype(f32) * (1.0 / 1048576.0)
    bias = jnp.log2(weight.astype(f32) * (1.0 / 16.0)) - RATE2 * jnp.sum(p * p, axis=0, keepdims=True)
    hi, lo = split(p)
    return jnp.concatenate([hi, lo], 0).T, jnp.concatenate([hi, ext_rows(bias, True)], 0).T


def body(t_hbm, g_hbm, w_hbm, out_ref, tbuf, sbuf, lhs, rhs, acc, part, got,
         loc_sem, ss, sr, ts, tr, fs, fr, ps, pr, ready):
    me = coords()
    z, x, y, c = me
    local = [
        pltpu.make_async_copy(g_hbm, sbuf.at[0, pl.ds(0, D)], loc_sem.at[0]),
        pltpu.make_async_copy(w_hbm, sbuf.at[0, pl.ds(D, 1)], loc_sem.at[1]),
        pltpu.make_async_copy(t_hbm, tbuf.at[0], loc_sem.at[2]),
    ]
    for cp in local:
        cp.start()
    bar = pltpu.get_barrier_semaphore()
    axes = ("dx", "dy", "dz")
    lower = {}
    for name, v in zip(axes, (x, y, z)):
        for k in (1, 3, 2):
            lower[name, k] = lax.rem(v + k, 4) < v if name == "dz" else rank(lax.rem(v + k, 4)) < rank(v)
    for (name, k), low in lower.items():
        @pl.when(jnp.logical_not(low))
        def _():
            pl.semaphore_signal(bar, 1, device_id=peer(me, **{name: k}), device_id_type=MESH)

    @pl.when(c == 1)
    def _():
        pl.semaphore_signal(bar, 1, device_id=peer(me, dc=1), device_id_type=MESH)

    acc[...] = jnp.zeros_like(acc)
    count = 1 - c
    for low in lower.values():
        count = count + low.astype(i32)

    @pl.when(count > 0)
    def _():
        pl.semaphore_wait(bar, count)

    for (name, k), low in lower.items():
        @pl.when(low)
        def _():
            pl.semaphore_signal(ready.at[axes.index(name), 4 - k], 1, device_id=peer(me, **{name: k}), device_id_type=MESH)

    @pl.when(c == 0)
    def _():
        pl.semaphore_signal(ready.at[0, 0], 1, device_id=peer(me, dc=1), device_id_type=MESH)

    for cp in local:
        cp.wait()

    def copy(src, dst, s, r, **to):
        return pltpu.make_async_remote_copy(src_ref=src, dst_ref=dst, send_sem=s, recv_sem=r, device_id=peer(me, **to), device_id_type=MESH)

    def send(*args, **to):
        cp = copy(*args, **to)
        cp.start()
        return cp

    def rows(k):
        return sbuf.at[k, pl.ds(0, D + 1)]

    sends, tsend, tfwd = {}, {}, {}

    def first(k):
        return dict(dx=k * (1 - c), dy=k * c)

    def second(k):
        return dict(dx=k * c, dy=k * (1 - c))

    def relay(k):
        for j in (2, 1, 3):
            n = 4 * k + j
            sends[n] = send(rows(4 * k), rows(n), ss.at[n], sr.at[n], **second(j))

    opening = []
    for k in (1, 3, 2):
        lx, ly = lower["dx", k], lower["dy", k]
        sends[4 * k] = copy(rows(0), rows(4 * k), ss.at[4 * k], sr.at[4 * k], **first(k))
        sends[k] = copy(rows(0), rows(k), ss.at[k], sr.at[k], **second(k))
        tsend[k] = copy(tbuf.at[0], tbuf.at[2 * k], ts.at[k], tr.at[k], dz=k)
        opening.append((0, sends[4 * k], jnp.logical_or(jnp.logical_and(c == 0, lx), jnp.logical_and(c == 1, ly)), ready.at[c, k]))
        opening.append((0, sends[k], jnp.logical_or(jnp.logical_and(c == 1, lx), jnp.logical_and(c == 0, ly)), ready.at[1 - c, k]))
        opening.append((1, tsend[k], lower["dz", k], ready.at[2, k]))
    opening.sort(key=lambda o: o[0])
    for _, cp, low, _ in opening:
        @pl.when(low)
        def _():
            cp.start()

    @pl.when(c == 1)
    def _():
        pl.semaphore_wait(ready.at[0, 0], 1)

    tfwd[0] = send(tbuf.at[0], tbuf.at[1], fs.at[0], fr.at[0], dc=1)
    for _, cp, low, sem in opening:
        @pl.when(jnp.logical_not(low))
        def _():
            pl.semaphore_wait(sem, 1)
            cp.start()

    def prep_t(i):
        rhs[:, pl.ds(i * TGT, TGT)] = prep_targets(tbuf[i])

    def prep_s(n):
        k = SLOTS[n]
        a, e = prep_sources(sbuf[k, 0:D], sbuf[k, D:D + 1])
        lhs[pl.ds(n * SRC, SRC), 0:128] = a
        lhs[pl.ds(n * SRC, SRC), 128:256] = e

    def lanes(i, w):
        return pl.ds(i * TGT if isinstance(i, int) else pl.multiple_of(i * TGT, TGT), w * TGT)

    def unit(lo, hi, i, w=2):
        n = (hi - lo) * SRC
        x = jnp.dot(lhs[pl.ds(lo * SRC, n), :], rhs[:, lanes(i, w)], preferred_element_type=f32)
        e = jnp.exp2(x)
        acc[:, lanes(i, w)] += e.reshape(n // 8, 8, w * TGT).sum(0)

    def group(lo, hi):
        for n in range(lo, hi):
            if SLOTS[n] % 4:
                sends[SLOTS[n]].wait_recv()
        for n in range(lo, hi):
            prep_s(n)

    def part_copy(i, dz, dc):
        return pltpu.make_async_remote_copy(src_ref=part.at[i], dst_ref=got.at[i], send_sem=ps.at[i], recv_sem=pr.at[i], device_id=peer(me, dz=dz, dc=dc), device_id_type=MESH)

    def reduce_part(i):
        part[i] = jnp.sum(acc[:, lanes(i, 1)], axis=0, keepdims=True)

    slots = []
    for u in range(3):
        zt = u + (u >= me[0]).astype(i32)
        slots.append(2 * lax.rem(me[0] - zt + 4, 4))

    prep_t(0)
    for k in (1, 3, 2):
        sends[4 * k].wait_recv()
        relay(k)
    group(0, EARLY)
    unit(0, EARLY, 0, 1)
    tfwd[0].wait_recv()
    prep_t(1)
    unit(0, EARLY, 1, 1)
    for dz in ZS_ARRIVE:
        tsend[dz].wait_recv()
        tfwd[dz] = send(tbuf.at[2 * dz], tbuf.at[2 * dz + 1], fs.at[dz], fr.at[dz], dc=1)
        prep_t(2 * dz)
        unit(0, EARLY, 2 * dz, 1)
    for dz in ZS_ARRIVE:
        tfwd[dz].wait_recv()
        prep_t(2 * dz + 1)
        unit(0, EARLY, 2 * dz + 1, 1)
    for lo, hi in LATE:
        group(lo, hi)
        unit(lo, hi, slots[0])
    for u, i in enumerate(slots):
        if u:
            unit(EARLY, 16, i)
        reduce_part(i)
        reduce_part(i + 1)
        for dc in range(2):
            part_copy(i + dc, lax.rem(4 - lax.div(i, 2), 4), dc).start()
    unit(EARLY, 16, 0)
    reduce_part(1)
    part_copy(1, 0, 1).start()
    for cp in list(sends.values()) + list(tsend.values()) + list(tfwd.values()):
        cp.wait_send()
    total = jnp.sum(acc[:, lanes(0, 1)], axis=0, keepdims=True)
    for i in range(1, 8):
        part_copy(i, 0, 1).wait_send()
    for i in range(1, 8):
        part_copy(i, 0, 1).wait_recv()
        total = total + got[i]
    out_ref[...] = total


def shards(targets, source_grid, source_weight):
    any_spec = pl.BlockSpec(memory_space=pltpu.HBM)
    targets, source_grid, source_weight = (pltpu.with_memory_space_constraint(v, pltpu.HBM) for v in (targets, source_grid, source_weight))
    out = pl.pallas_call(
        body,
        out_shape=jax.ShapeDtypeStruct((1, TGT), f32),
        in_specs=[any_spec] * 3,
        out_specs=pl.BlockSpec(memory_space=pltpu.VMEM),
        scratch_shapes=[
            pltpu.VMEM((8, D, TGT), f32),
            pltpu.VMEM((16, D + 8, SRC), i32),
            pltpu.VMEM((16 * SRC, 256), bf16),
            pltpu.VMEM((256, 8 * TGT), bf16),
            pltpu.VMEM((8, 8 * TGT), f32),
            pltpu.VMEM((8, 1, TGT), f32),
            pltpu.VMEM((8, 1, TGT), f32),
            DMA((3,)), DMA((16,)), DMA((16,)), DMA((4,)), DMA((4,)), DMA((4,)), DMA((4,)), DMA((8,)), DMA((8,)), pltpu.SemaphoreType.REGULAR((3, 4)),
        ],
        compiler_params=pltpu.CompilerParams(collective_id=0, has_side_effects=True, vmem_limit_bytes=24 * 1024 * 1024),
    )(targets, source_grid, source_weight)
    return out.reshape(TGT)


def solution(mesh):
    in_specs = (P(None, ("grp", "dev")), P(None, ("grp", "dev")), P(None, ("grp", "dev")))
    return jax.shard_map(shards, mesh=mesh, in_specs=in_specs, out_specs=P(("grp", "dev")), check_vma=False)
```
